512 devices in a mesh: ep: 32 (over z, x), fsdp: 16 (over y, core).
Axes of the slice: x: 4, y: 8, z: 8, core: 2. Of those that a mesh axis runs over, the one named last changes fastest.
Arguments:
- train_down: float32 [64, 1408, 2048], P('ep', None, 'fsdp'), may hold values from -0.21875 to 0.21875
- other_down: float32 [64, 1408, 2048], P('ep', None, 'fsdp'), may hold values from -0.15625 to 0.15625
- router_weight: float32 [2048, 64], P('fsdp', 'ep'), may hold values from -0.125 to 0.125
- router_gain: float32 [2048], P('fsdp'), may hold values from 0.25 to 1.75
Outputs:
- ready_down: bfloat16 [64, 1408, 2048], P('ep')
- scale_down: float32 [64, 1408], P('ep')
- serve_router: bfloat16 [2048, 64], replicated
- latest_down: float32 [64, 1408, 2048], P('ep', None, 'fsdp')
The draws below stay inside these ranges and needn't reach their ends.
All inputs are finite; a program needn't handle non-finite values.
Results may differ from the reference program's by a relative error of at most 0.001.
Values may be sent and summed in bfloat16 or wider, within the bound.
A program may use at most 128 MiB of HBM per device.

```python
import jax
import jax.numpy as jnp
from jax import lax

EXPERTS = 64
D_MODEL = 2048
D_EXPERT = 1408


def raised(values, stream_key, source, target, shards_of, factor):
    def block_of(axis_at):
        return (jnp.arange(values.shape[axis_at]) // (values.shape[axis_at] // shards_of)).reshape((-1,) + (1,) * (values.ndim - 1 - axis_at))

    first = jax.random.permutation(stream_key, shards_of)[block_of(target)]
    other_side = (block_of(target) + shards_of // 2) % shards_of
    return jnp.where((block_of(source) == first) | (block_of(source) == other_side), factor * values, values)


def levels(own_key, dims, pieces, smallest, top_value):
    level = 1.0
    for dim, shards_of in pieces:
        heights = jax.random.uniform(jax.random.fold_in(jax.random.fold_in(own_key, 6), dim), (shards_of,), jnp.float32, smallest / len(pieces), top_value / len(pieces))
        level = level * jnp.repeat(jnp.exp(heights), dims[dim] // shards_of).reshape((-1,) + (1,) * (len(dims) - 1 - dim))
    return level


def scatter_about(rng, dims, spread, bound, cuts=(), held_as=jnp.bfloat16):
    gain = levels(rng, dims, cuts, -0.22, 0.18) if cuts else 1.0
    array = jax.random.normal(rng, dims, jnp.float32) * spread * gain
    return jnp.minimum(jnp.maximum(array, -bound), bound).astype(held_as)


def heavy_noise(key, extent, spread, limit, pieces, heavy, kind=jnp.bfloat16):
    drawn = spread * jax.random.normal(key, extent, jnp.float32)
    if pieces:
        drawn = drawn * levels(key, extent, pieces, -0.22, 0.18)
    return jnp.clip(raised(drawn, jax.random.fold_in(key, 3), *heavy), -limit, limit).astype(kind)


def setup_inputs(seed: int = 0) -> dict:
    arg_keys = jax.random.split(jax.random.key(seed), 5)
    return {
        "train_down": heavy_noise(arg_keys[0], (EXPERTS, D_EXPERT, D_MODEL), D_EXPERT ** -0.5, 0.21875, ((0, 32), (2, 16)), (2, 1, 16, 2.0), jnp.float32),
        "other_down": scatter_about(arg_keys[1], (EXPERTS, D_EXPERT, D_MODEL), D_EXPERT ** -0.5, 0.15625, ((0, 32), (2, 16)), jnp.float32),
        "router_weight": scatter_about(arg_keys[2], (D_MODEL, EXPERTS), D_MODEL ** -0.5, 0.125, ((0, 16), (1, 32)), jnp.float32),
        "router_gain": jnp.clip(1.0 + 0.15 * jax.random.normal(arg_keys[3], (D_MODEL,), jnp.float32), 0.25, 1.75),
    }


def reference(train_down, other_down, router_weight, router_gain):
    latest_down = 0.5 * other_down + 0.5 * train_down
    scale_down = jnp.sqrt(lax.optimization_barrier(jnp.sum(latest_down * latest_down, axis=2)))
    ready_down = (latest_down / jnp.expand_dims(scale_down, 2)).astype(jnp.bfloat16)
    serve_router = (router_weight * router_gain[:, None]).astype(jnp.bfloat16)
    return (ready_down, scale_down, serve_router, latest_down)
```

```python
import functools

import jax
import jax.numpy as jnp
from jax import lax
from jax.experimental import pallas as pl
from jax.experimental.pallas import tpu as pltpu
from jax.sharding import PartitionSpec as P

MESH = pl.DeviceIdType.MESH
LANES = 128
CHUNKS = 8


def gather_kernel(
    ny, nz, nx, rows,
    train_ref, other_ref, weight_ref, gain_ref,
    land, scale_ref, router_ref, latest_ref,
    train_buf, other_buf, w_buf, g_buf, mine, sums, inverse, part, rland, load_sem, sum_send, sum_recv, ring_send, ring_recv,
    twin_send, twin_recv, rt_send, rt_recv, z_send, z_recv, x_send, x_recv,
):
    n = 2 * ny
    half = ny // 2
    total_rows = 2 * rows
    span = total_rows // CHUNKS
    groups = total_rows // 8
    vregs = (groups + LANES - 1) // LANES
    f_me = lax.axis_index("fsdp")
    e_me = lax.axis_index("ep")
    y, core = f_me // 2, lax.rem(f_me, 2)
    z, x = e_me // nx, lax.rem(e_me, nx)

    def column(y_index, core_index):
        return {"fsdp": y_index * 2 + core_index}

    right = column(lax.rem(y + 1, ny), core)
    left = column(lax.rem(y + ny - 1, ny), core)
    twin = column(y, 1 - core)
    peers = [lax.rem(f_me + d, n) for d in range(1, n)]
    z_peers = [lax.rem(z + d, nz) * nx + x for d in range(1, nz)]
    x_peers = [z * nx + lax.rem(x + d, nx) for d in range(1, nx)]

    def chunk(k):
        return pl.ds(pl.multiple_of(k * span, 16), span)

    small = (
        pltpu.make_async_copy(weight_ref, w_buf, load_sem.at[2 * CHUNKS]),
        pltpu.make_async_copy(gain_ref, g_buf, load_sem.at[2 * CHUNKS + 1]),
    )
    loads = []
    for k in range(CHUNKS):
        at = pl.ds(k * span, span)
        a = pltpu.make_async_copy(train_ref.at[at], train_buf.at[at], load_sem.at[2 * k])
        b = pltpu.make_async_copy(other_ref.at[at], other_buf.at[at], load_sem.at[2 * k + 1])
        a.start()
        b.start()
        loads.append((a, b))
    for c in small:
        c.start()

    barrier = pltpu.get_barrier_semaphore()
    for p in peers:
        pl.semaphore_signal(barrier, inc=1, device_id={"fsdp": p}, device_id_type=MESH)
    for p in z_peers + x_peers:
        pl.semaphore_signal(barrier, inc=1, device_id={"ep": p}, device_id_type=MESH)

    lane = lax.broadcasted_iota(jnp.int32, (8, LANES), 1)
    packed = None
    for g in range(groups):
        if g * 8 % span == 0:
            for c in loads[g * 8 // span]:
                c.wait()
        at = pl.ds(g * 8, 8)
        value = 0.5 * other_buf[at, :] + 0.5 * train_buf[at, :]
        latest_ref[at, :] = value
        total = jnp.sum(value * value, axis=1, keepdims=True)
        if g % LANES == 0:
            packed = jnp.ones((8, LANES), jnp.float32)
        packed = jnp.where(lane == g % LANES, total, packed)
        if g % LANES == LANES - 1 or g == groups - 1:
            mine[g // LANES] = packed
    for c in small:
        c.wait()
    part[...] = w_buf[...] * g_buf[...]

    pl.semaphore_wait(barrier, len(peers) + len(z_peers) + len(x_peers))

    def sum_copy(d, m):
        words = pl.ds(0, 1) if m == 0 else pl.ds(1, vregs - 1)
        return pltpu.make_async_remote_copy(
            mine.at[words], sums.at[f_me, words], sum_send.at[2 * d + m], sum_recv.at[2 * d + m],
            device_id={"fsdp": peers[d]}, device_id_type=MESH,
        )

    def router_copy(d):
        return pltpu.make_async_remote_copy(
            part, rland.at[z, x, f_me], rt_send.at[d], rt_recv.at[d],
            device_id={"fsdp": peers[d]}, device_id_type=MESH,
        )

    messages = 1 if vregs == 1 else 2
    far_first = sorted(range(n - 1), key=lambda d: -min(d + 1, n - 1 - d))
    for m in range(messages):
        for d in far_first:
            sum_copy(d, m).start()
    for d in far_first:
        router_copy(d).start()
    for m in range(vregs):
        sums[f_me, m] = mine[m]
    rland[z, x, f_me] = part[...]

    def ring_copy(way, hop, k, origin):
        block = land.at[2 * origin + core, chunk(k)]
        return pltpu.make_async_remote_copy(
            block, block, ring_send.at[way, hop - 1], ring_recv.at[way, hop - 1, k],
            device_id=right if way == 0 else left, device_id_type=MESH,
        )

    def twin_copy(hop, k, origin):
        block = land.at[2 * origin + core, chunk(k)]
        return pltpu.make_async_remote_copy(
            block, block, twin_send.at[hop], twin_recv.at[hop],
            device_id=twin, device_id_type=MESH,
        )

    done = 0
    for k in range(CHUNKS):
        need = ((k + 1) * span // 8 + LANES - 1) // LANES
        while done < need:
            m = 0 if done == 0 else 1
            if done < 2:
                for d in range(n - 1):
                    sum_copy(d, m).wait_recv()
            for v in range(done, 1 if m == 0 else vregs):
                total = sums[0, v]
                for s in range(1, n):
                    total = total + sums[s, v]
                scale = jnp.sqrt(total)
                mine_scale = scale
                inverse[0, v] = mine_scale
                inverse[1, v] = 1.0 / scale
            done = 1 if m == 0 else vregs
        for r in range(k * span // 16, (k + 1) * span // 16):
            both = []
            for g in (2 * r, 2 * r + 1):
                inv = inverse[1, g // LANES][:, g % LANES : g % LANES + 1]
                both.append(latest_ref[pl.ds(8 * g, 8), :] * jnp.broadcast_to(inv, (8, LANES)))
            land[f_me, pl.ds(16 * r, 16), :] = jnp.concatenate(both, axis=0).astype(jnp.bfloat16)
        ring_copy(0, 1, k, y).start()
        ring_copy(1, 1, k, y).start()
        twin_copy(0, k, y).start()

    for d in range(n - 1):
        router_copy(d).wait_recv()

    def z_copy(d):
        block = rland.at[z, x]
        return pltpu.make_async_remote_copy(
            block, block, z_send.at[d], z_recv.at[d], device_id={"ep": z_peers[d]}, device_id_type=MESH,
        )

    def x_copy(d):
        block = rland.at[:, x]
        return pltpu.make_async_remote_copy(
            block, block, x_send.at[d], x_recv.at[d], device_id={"ep": x_peers[d]}, device_id_type=MESH,
        )

    for d in range(nz - 1):
        z_copy(d).start()

    def origin_of(way, hop):
        return lax.rem(y + (ny - hop if way == 0 else hop), ny)

    def arrival(way, hop, k, onward):
        origin = origin_of(way, hop)
        ring_copy(way, hop, k, origin).wait_recv()
        if onward:
            ring_copy(way, hop + 1, k, origin).start()
        twin_copy(2 * hop + way if hop < half else 2 * half, k, origin).start()

    for hop in range(1, half):
        split = CHUNKS // 2
        last = hop == half - 1

        def first(k, c):
            arrival(0, hop, k, True)
            arrival(1, hop, k, not last)
            return c

        def second(k, c):
            arrival(0, hop, k, not last)
            arrival(1, hop, k, True)
            return c

        lax.fori_loop(0, split, first, 0)
        lax.fori_loop(split, CHUNKS, second, 0)
        if hop == 1:
            for d in range(nz - 1):
                z_copy(d).wait_recv()
            for d in range(nx - 1):
                x_copy(d).start()
            rows_at = lax.broadcasted_iota(jnp.int32, (LANES, LANES), 0)
            lanes_at = lax.broadcasted_iota(jnp.int32, (LANES, LANES), 1)
            for t in range(total_rows // LANES):
                tile = jnp.concatenate(
                    [
                        jnp.broadcast_to(inverse[0, g // LANES][:, g % LANES : g % LANES + 1], (8, LANES))
                        for g in range(16 * t, 16 * t + 16)
                    ],
                    axis=0,
                )
                line = jnp.sum(jnp.where(rows_at == lanes_at, tile, 0.0), axis=0, keepdims=True)
                e, at = divmod(t * LANES, rows)
                scale_ref[pl.ds(e, 1), pl.ds(at, LANES)] = line
    for d in range(nx - 1):
        x_copy(d).wait_recv()

    def lines(f, c):
        for q in range(nz * nx // 8):
            block = jnp.concatenate([rland[(8 * q + i) // nx, (8 * q + i) % nx, f] for i in range(8)], axis=0)
            router_ref[pl.ds(16 * q, 16), pl.ds(pl.multiple_of(f * LANES, LANES), LANES)] = block.astype(jnp.bfloat16)
        return c

    lax.fori_loop(0, n, lines, 0)

    def final(k, c):
        arrival(0, half, k, False)
        arrival(1, half, k + CHUNKS // 2, False)
        return c

    lax.fori_loop(0, CHUNKS // 2, final, 0)

    def whole(sem_send, sem_recv, part_rows):
        block = land.at[0, pl.ds(0, part_rows)]
        return pltpu.make_async_remote_copy(block, block, sem_send, sem_recv, device_id=twin, device_id_type=MESH)

    for hop in range(2 * half + 1):
        if hop == 1:
            continue
        whole(twin_send.at[hop], twin_recv.at[hop], total_rows).wait()
    for way in range(2):
        for hop in range(1, half + 1):
            part_rows = total_rows if hop < half else total_rows // 2
            whole(ring_send.at[way, hop - 1], twin_recv.at[0], part_rows).wait_send()
    for d in range(n - 1):
        for m in range(messages):
            sum_copy(d, m).wait_send()
        router_copy(d).wait_send()
    for d in range(nz - 1):
        z_copy(d).wait_send()
    for d in range(nx - 1):
        x_copy(d).wait_send()


def write_kernel(land, scale_in, router_in, latest_in, ready, scale, router, latest, sem):
    n = land.shape[0]
    copies = [
        pltpu.make_async_copy(land.at[f], ready.at[:, pl.ds(f * LANES, LANES)], sem.at[f]) for f in range(n)
    ]
    copies.append(pltpu.make_async_copy(scale_in, scale, sem.at[n]))
    copies.append(pltpu.make_async_copy(router_in, router, sem.at[n + 1]))
    copies.append(pltpu.make_async_copy(latest_in, latest, sem.at[n + 2]))
    for c in copies:
        c.start()
    for c in copies:
        c.wait()


def solution(mesh, nx=4):
    ep, n = mesh.shape["ep"], mesh.shape["fsdp"]
    ny, nz = n // 2, ep // nx

    def on_device(train_down, other_down, router_weight, router_gain):
        experts, rows, width = train_down.shape
        total_rows = experts * rows
        vregs = (total_rows // 8 + LANES - 1) // LANES
        f32, bf16 = jnp.float32, jnp.bfloat16
        half = ny // 2
        vmem = lambda shape, dtype: pltpu.VMEM(shape, dtype)
        dma = lambda *shape: pltpu.SemaphoreType.DMA(shape)
        anywhere = pl.BlockSpec(memory_space=pl.ANY)
        in_vmem = pl.BlockSpec(memory_space=pltpu.VMEM)
        results = pl.pallas_call(
            functools.partial(gather_kernel, ny, nz, nx, rows),
            out_shape=(
                pltpu.VMEM((n, total_rows, width), bf16),
                pltpu.VMEM((experts, rows), f32),
                pltpu.VMEM((ep * experts, n * width), bf16),
                pltpu.VMEM((total_rows, width), f32),
            ),
            in_specs=[pl.BlockSpec(memory_space=pltpu.HBM)] * 4,
            out_specs=(in_vmem,) * 4,
            scratch_shapes=[
                vmem((total_rows, width), f32),
                vmem((total_rows, width), f32),
                vmem((experts, width), f32),
                vmem((1, width), f32),
                vmem((vregs, 8, LANES), f32),
                vmem((n, vregs, 8, LANES), f32),
                vmem((2, vregs, 8, LANES), f32),
                vmem((experts, width), f32),
                vmem((nz, nx, n, experts, width), f32),
                dma(2 * CHUNKS + 2),
                dma(2 * (n - 1)),
                dma(2 * (n - 1)),
                dma(2, half),
                dma(2, half, CHUNKS),
                dma(2 * half + 1),
                dma(2 * half + 1),
                dma(n - 1),
                dma(n - 1),
                dma(nz),
                dma(nz),
                dma(nx),
                dma(nx),
            ],
            compiler_params=pltpu.CompilerParams(
                collective_id=0, has_side_effects=True, vmem_limit_bytes=24 * 1024 * 1024
            ),
            name="gather",
        )(
            *(
                pltpu.with_memory_space_constraint(a, pltpu.HBM)
                for a in (
                    train_down.reshape(total_rows, width),
                    other_down.reshape(total_rows, width),
                    router_weight.T,
                    router_gain.reshape(1, width),
                )
            )
        )
        held = [pltpu.with_memory_space_constraint(r, pltpu.VMEM) for r in results]
        ready, scale, router, latest = pl.pallas_call(
            write_kernel,
            out_shape=(
                jax.ShapeDtypeStruct((total_rows, n * width), bf16),
                jax.ShapeDtypeStruct((experts, rows), f32),
                jax.ShapeDtypeStruct((ep * experts, n * width), bf16),
                jax.ShapeDtypeStruct((total_rows, width), f32),
            ),
            in_specs=[in_vmem] * 4,
            out_specs=(anywhere,) * 4,
            scratch_shapes=[dma(n + 3)],
            compiler_params=pltpu.CompilerParams(vmem_limit_bytes=1024 * 1024),
            name="write",
        )(*held)
        return (
            ready.reshape(experts, rows, n * width),
            scale,
            router.T,
            latest.reshape(experts, rows, width),
        )

    placed = (P("ep", None, "fsdp"), P("ep", None, "fsdp"), P("fsdp", "ep"), P("fsdp"))
    return jax.shard_map(
        on_device,
        mesh=mesh,
        in_specs=placed,
        out_specs=(P("ep", None, None), P("ep", None), P(), P("ep", None, "fsdp")),
        check_vma=False,
    )
```

```python
import functools

import jax
import jax.numpy as jnp
from jax import lax
from jax.experimental import pallas as pl
from jax.experimental.pallas import tpu as pltpu
from jax.sharding import PartitionSpec as P

MESH = pl.DeviceIdType.MESH
LANES = 128
CHUNKS = 16
EARLY = 6
RANGE = 240.0
TINY = 1e-36
TURNS = (3, 6, 9, 12, 13, 19, 26)
LN2 = 0.6931471805599453


def gather_kernel(
    ny, nz, nx, rows,
    train_ref, other_ref, weight_ref, gain_ref,
    land, scale_ref, router_ref, latest_ref,
    train_buf, other_buf, w_buf, g_buf, code, sums, inverse, factor, rland, load_sem, sum_send, sum_recv, ring_send, ring_recv,
    twin_send, twin_recv, tsum_send, tsum_recv, tcode_send, tcode_recv, z_send, z_recv, x_send, x_recv,
):
    n = 2 * ny
    half = ny // 2
    total_rows = 2 * rows
    span = total_rows // CHUNKS
    early_rows = EARLY * span
    groups = total_rows // 8
    vregs = (groups + LANES - 1) // LANES
    f_me = lax.axis_index("fsdp")
    e_me = lax.axis_index("ep")
    y, core = f_me // 2, lax.rem(f_me, 2)
    z, x = e_me // nx, lax.rem(e_me, nx)

    def column(y_index, core_index):
        return {"fsdp": y_index * 2 + core_index}

    right = column(lax.rem(y + 1, ny), core)
    left = column(lax.rem(y + ny - 1, ny), core)
    twin = column(y, 1 - core)
    z_next = {"ep": lax.rem(z + 1, nz) * nx + x}
    z_last = {"ep": lax.rem(z + nz - 1, nz) * nx + x}
    x_next = {"ep": z * nx + lax.rem(x + 1, nx)}
    x_last = {"ep": z * nx + lax.rem(x + nx - 1, nx)}
    neighbours = [right, left, twin] + ([z_next, z_last] if nz > 1 else []) + ([x_next, x_last] if nx > 1 else [])

    small = (
        pltpu.make_async_copy(weight_ref, w_buf, load_sem.at[2 * CHUNKS]),
        pltpu.make_async_copy(gain_ref, g_buf, load_sem.at[2 * CHUNKS + 1]),
    )
    loads = []
    for k in range(CHUNKS):
        at = pl.ds(k * span, span)
        a = pltpu.make_async_copy(train_ref.at[at], train_buf.at[at], load_sem.at[2 * k])
        b = pltpu.make_async_copy(other_ref.at[at], other_buf.at[at], load_sem.at[2 * k + 1])
        a.start()
        b.start()
        loads.append((a, b))
        if k == 0:
            for c in small:
                c.start()

    barrier = pltpu.get_barrier_semaphore()
    for p in neighbours:
        pl.semaphore_signal(barrier, inc=1, device_id=p, device_id_type=MESH)

    def origin_of(way, hop):
        return lax.rem(y + (ny - hop if way == 0 else hop), ny)

    def apart(way, hop):
        return 0 if hop == 0 else (ny - hop if way == 0 else hop)

    def piece(k, origin, early):
        buf = code if early else land
        return buf.at[2 * origin + core, pl.ds(pl.multiple_of(k * span, 16), span)]

    def ring_copy(way, hop, k, early):
        block = piece(k, origin_of(way, hop - 1), early)
        return pltpu.make_async_remote_copy(
            block, block, ring_send.at[way, hop - 1], ring_recv.at[way, hop - 1, k],
            device_id=right if way == 0 else left, device_id_type=MESH,
        )

    def ring_wait(way, hop, k, early):
        block = piece(k, origin_of(way, hop), early)
        pltpu.make_async_remote_copy(
            block, block, ring_send.at[way, hop - 1], ring_recv.at[way, hop - 1, k],
            device_id=right if way == 0 else left, device_id_type=MESH,
        ).wait_recv()

    def twin_copy(way, hop, k, early):
        block = piece(k, origin_of(way, hop), early)
        d = apart(way, hop)
        return pltpu.make_async_remote_copy(
            block, block, (tcode_send if early else twin_send).at[d], (tcode_recv if early else twin_recv).at[d],
            device_id=twin, device_id_type=MESH,
        )

    def launch(k, early):
        ring_copy(0, 1, k, early).start()
        ring_copy(1, 1, k, early).start()
        twin_copy(0, 0, k, early).start()

    def arrival(way, hop, k, early, onward):
        ring_wait(way, hop, k, early)
        if onward:
            ring_copy(way, hop + 1, k, early).start()
        twin_copy(way, hop, k, early).start()

    def sum_copy(way, hop):
        block = sums.at[2 * origin_of(way, hop - 1) + core]
        return pltpu.make_async_remote_copy(
            block, block, sum_send.at[way, hop - 1], sum_recv.at[way, hop - 1],
            device_id=right if way == 0 else left, device_id_type=MESH,
        )

    def sum_wait(way, hop):
        block = sums.at[2 * origin_of(way, hop) + core]
        pltpu.make_async_remote_copy(
            block, block, sum_send.at[way, hop - 1], sum_recv.at[way, hop - 1],
            device_id=right if way == 0 else left, device_id_type=MESH,
        ).wait_recv()

    def sum_twin(d, whose):
        block = sums.at[2 * lax.rem(y + d, ny) + whose]
        return pltpu.make_async_remote_copy(
            block, block, tsum_send.at[d], tsum_recv.at[d], device_id=twin, device_id_type=MESH,
        )

    lane = lax.broadcasted_iota(jnp.int32, (8, LANES), 1)
    ones = jnp.ones((8, LANES), jnp.float32)
    words = [ones]

    def sweep(k):
        for c in loads[k]:
            c.wait()
        both = []
        for g in range(k * span // 8, (k + 1) * span // 8):
            at = pl.ds(g * 8, 8)
            value = 0.5 * other_buf[at, :] + 0.5 * train_buf[at, :]
            latest_ref[at, :] = value
            total = jnp.sum(value * value, axis=1, keepdims=True)
            words[0] = jnp.where(lane == g % LANES, total, words[0])
            if g % LANES == LANES - 1 or g == groups - 1:
                sums[f_me, g // LANES] = words[0]
                words[0] = ones
            if k < EARLY:
                reach = RANGE * lax.rsqrt(jnp.maximum(jnp.broadcast_to(total, (8, LANES)), TINY))
                size = jnp.exp(LN2 * (jnp.abs(value) * reach - RANGE / 2))
                both.append(jnp.where(value < 0, -size, size))
                if len(both) == 2:
                    code[f_me, pl.ds((g - 1) * 8, 16), :] = jnp.concatenate(both, axis=0).astype(jnp.bfloat16)
                    both = []

    sweep(0)
    pl.semaphore_wait(barrier, len(neighbours))
    launch(0, True)
    sweep(1)
    launch(1, True)
    for k in range(2, CHUNKS):
        sweep(k)
        if k == 2:
            for c in small:
                c.wait()
            sums[f_me, vregs, pl.ds(0, 2), :] = w_buf[...] * g_buf[...]
    sum_copy(0, 1).start()
    sum_copy(1, 1).start()
    sum_twin(0, core).start()
    for k in range(2, min(4, EARLY)):
        launch(k, True)

    mid = EARLY // 2

    def early_step(hop, k):
        last = hop == half - 1
        arrival(0, hop, k, True, not last or k < mid)
        arrival(1, hop, k, True, not last or k >= mid)

    waiting = [(0, k) for k in range(4, EARLY)] + [(hop, k) for hop in range(1, half) for k in range(EARLY)]

    ahead = []

    def early_some(count):
        ahead.extend(waiting[:count])
        for hop, k in waiting[:count]:
            if hop == 0:
                launch(k, True)
            else:
                early_step(hop, k)
        del waiting[:count]

    for hop in range(1, half + 1):
        sum_wait(0, hop)
        if hop < half:
            sum_copy(0, hop + 1).start()
            sum_wait(1, hop)
            if hop < half - 1:
                sum_copy(1, hop + 1).start()
            sum_twin(apart(1, hop), core).start()
        sum_twin(apart(0, hop), core).start()
        early_some(3)
    for d in range(ny):
        sum_twin(d, 1 - core).wait_recv()

    for v in range(vregs):
        total = sums[0, v]
        for s in range(1, n):
            total = total + sums[s, v]
        scale = jnp.sqrt(total)
        inverse[0, v] = scale
        inverse[1, v] = 1.0 / scale

    def scaled(r):
        both = []
        for g in (2 * r, 2 * r + 1):
            inv = inverse[1, g // LANES][:, g % LANES : g % LANES + 1]
            both.append(latest_ref[pl.ds(8 * g, 8), :] * jnp.broadcast_to(inv, (8, LANES)))
        land[f_me, pl.ds(16 * r, 16), :] = jnp.concatenate(both, axis=0).astype(jnp.bfloat16)

    for k in range(EARLY, CHUNKS):
        for r in range(k * span // 16, (k + 1) * span // 16):
            scaled(r)
        launch(k, False)
    sent = {(hop + 1, k) for hop, k in ahead}
    first = [(hop, k) for hop, k in waiting if hop == 1 or (hop, k) in sent]
    second = [step for step in waiting if step not in first]
    for hop, k in first:
        early_step(hop, k)

    for f in range(n):
        rland[z, x, f] = sums[f, vregs, pl.ds(0, 2), :]

    def z_copy(way, step, where):
        block = rland.at[where, x]
        return pltpu.make_async_remote_copy(
            block, block, z_send.at[way, step], z_recv.at[way, step],
            device_id=z_last if way else z_next, device_id_type=MESH,
        )

    def x_copy(way, step, where):
        block = rland.at[:, where]
        return pltpu.make_async_remote_copy(
            block, block, x_send.at[way, step], x_recv.at[way, step],
            device_id=x_last if way else x_next, device_id_type=MESH,
        )

    def round_step(copy, size, me, step):
        for way, hops in enumerate((size // 2, size - 1 - size // 2)):
            where = lax.rem(me + size + (step if way else -step), size)
            if 1 <= step <= hops:
                copy(way, step - 1, where).wait_recv()
            if step < hops:
                copy(way, step, where).start()

    tasks = [functools.partial(round_step, z_copy, nz, z, step) for step in range(nz // 2 + 1)]
    tasks += [functools.partial(round_step, x_copy, nx, x, step) for step in range(nx // 2 + 1)]

    for s in range(n):
        for v in range(factor.shape[1]):
            factor[s, v] = jnp.sqrt(jnp.maximum(sums[s, v], TINY)) * inverse[1, v] * (1.0 / RANGE)
    for r in range(early_rows // 16):
        scaled(r)
    tasks.pop(0)()

    def decode(i):
        far = ((i >= ny - 2) & (i < 2 * ny - 3)) | (i == 2 * ny - 2)
        near = jnp.where(far, i - (ny - 2), i + 1)
        offset = jnp.where(i >= 2 * ny - 3, half, near + jnp.where(near >= half, 1, 0))
        slot = 2 * lax.rem(y + offset, ny) + jnp.where(far, 1 - core, core)

        @pl.when(far)
        def _():
            block = code.at[slot]
            pltpu.make_async_remote_copy(
                block, block, tcode_send.at[offset], tcode_recv.at[offset], device_id=twin, device_id_type=MESH,
            ).wait_recv()

        by = [factor[slot, v] for v in range(factor.shape[1])]
        for r in range(early_rows // 16):
            held = code[slot, pl.ds(16 * r, 16), :].astype(jnp.float32)
            size = jnp.log(jnp.abs(held)) * (1.0 / LN2) + RANGE / 2
            signed = jnp.where(held < 0, -size, size)
            part = jnp.concatenate(
                [
                    jnp.broadcast_to(by[g // LANES][:, g % LANES : g % LANES + 1], (8, LANES))
                    for g in (2 * r, 2 * r + 1)
                ],
                axis=0,
            )
            land[slot, pl.ds(16 * r, 16), :] = (signed * part).astype(jnp.bfloat16)

    late = CHUNKS - EARLY
    turn = EARLY + late // 2
    codes = n - 1

    def pair(hop, k, extra):
        if hop < half - 1:
            arrival(0, hop, k, False, True)
            arrival(1, hop, k, False, True)
        else:
            for way in range(2):
                ring_wait(way, hop, k, False)
                twin_copy(way, hop, k, False).start()

            @pl.when(k < turn)
            def _():
                ring_copy(0, hop + 1, k, False).start()

            @pl.when(k >= turn)
            def _():
                ring_copy(1, hop + 1, k, False).start()
        extra(k)

    def decode_step(base):
        def run(k):
            i = base + k - EARLY

            @pl.when(i < codes)
            def _():
                decode(i)

        return run

    due = {}
    for i, task in enumerate(tasks):
        if half == 1 or i >= len(TURNS):
            due.setdefault((half - 1, CHUNKS - 1), []).append(task)
        else:
            hop, k = divmod(TURNS[i], late)
            due.setdefault((min(hop + 1, half - 1), k + EARLY), []).append(task)

    for hop in range(1, half):

        def extra(k, hop=hop):
            for (at_hop, at), todo in due.items():
                if at_hop == hop:

                    @pl.when(k == at)
                    def _(todo=todo):
                        for task in todo:
                            task()

            if hop > 1:
                decode_step(late * (hop - 2))(k)

        def body(k, c, hop=hop, extra=extra):
            pair(hop, k, extra)
            return c

        lax.fori_loop(EARLY, CHUNKS, body, 0)
        if hop == 1:
            for early_hop, k in second:
                early_step(early_hop, k)
        if hop == min(2, half - 1):
            for k in range(mid):
                arrival(0, half, k, True, False)
                arrival(1, half, k + mid, True, False)
        if hop == 1:
            rows_at = lax.broadcasted_iota(jnp.int32, (LANES, LANES), 0)
            lanes_at = lax.broadcasted_iota(jnp.int32, (LANES, LANES), 1)
            for t in range(total_rows // LANES):
                tile = jnp.concatenate(
                    [
                        jnp.broadcast_to(inverse[0, g // LANES][:, g % LANES : g % LANES + 1], (8, LANES))
                        for g in range(16 * t, 16 * t + 16)
                    ],
                    axis=0,
                )
                line = jnp.sum(jnp.where(rows_at == lanes_at, tile, 0.0), axis=0, keepdims=True)
                e, at = divmod(t * LANES, rows)
                scale_ref[pl.ds(e, 1), pl.ds(at, LANES)] = line
    for i in range(late * (half - 2), codes):
        decode(jnp.int32(i))

    def lines(f, c):
        for q in range(nz * nx // 8):
            block = jnp.concatenate([rland[(8 * q + i) // nx, (8 * q + i) % nx, f] for i in range(8)], axis=0)
            router_ref[pl.ds(16 * q, 16), pl.ds(pl.multiple_of(f * LANES, LANES), LANES)] = block.astype(jnp.bfloat16)
        return c

    lax.fori_loop(0, n, lines, 0)

    def final(k, c):
        arrival(0, half, k, False, False)
        arrival(1, half, k + late // 2, False, False)
        return c

    lax.fori_loop(EARLY, turn, final, 0)

    def whole(buf, send, recv, part_rows):
        block = buf.at[0, pl.ds(0, part_rows)]
        return pltpu.make_async_remote_copy(block, block, send, recv, device_id=twin, device_id_type=MESH)

    for way in range(2):
        for hop in range(1, half + 1):
            part_rows = total_rows if hop < half else total_rows // 2
            whole(land, ring_send.at[way, hop - 1], twin_recv.at[0], part_rows).wait_send()
    for way in range(2):
        for hop in range(1, half + 1 - way):
            sum_copy(way, hop).wait_send()
    for d in range(ny):
        sum_twin(d, core).wait_send()
        whole(code, tcode_send.at[d], tcode_recv.at[d], early_rows).wait_send()
    for copy, size, me in ((z_copy, nz, z), (x_copy, nx, x)):
        for way, hops in enumerate((size // 2, size - 1 - size // 2)):
            for step in range(hops):
                copy(way, step, me).wait_send()
    for d in range(ny):
        whole(land, twin_send.at[d], twin_recv.at[d], total_rows - early_rows).wait()


def write_kernel(land, scale_in, router_in, latest_in, ready, scale, router, latest, sem):
    n = land.shape[0]
    copies = [
        pltpu.make_async_copy(land.at[f], ready.at[:, pl.ds(f * LANES, LANES)], sem.at[f]) for f in range(n)
    ]
    copies.append(pltpu.make_async_copy(scale_in, scale, sem.at[n]))
    copies.append(pltpu.make_async_copy(router_in, router, sem.at[n + 1]))
    copies.append(pltpu.make_async_copy(latest_in, latest, sem.at[n + 2]))
    for c in copies:
        c.start()
    for c in copies:
        c.wait()


def solution(mesh, nx=4):
    ep, n = mesh.shape["ep"], mesh.shape["fsdp"]
    ny, nz = n // 2, ep // nx

    def on_device(train_down, other_down, router_weight, router_gain):
        experts, rows, width = train_down.shape
        total_rows = experts * rows
        vregs = (total_rows // 8 + LANES - 1) // LANES
        f32, bf16 = jnp.float32, jnp.bfloat16
        half = ny // 2
        vmem = lambda shape, dtype: pltpu.VMEM(shape, dtype)
        dma = lambda *shape: pltpu.SemaphoreType.DMA(shape)
        anywhere = pl.BlockSpec(memory_space=pl.ANY)
        in_vmem = pl.BlockSpec(memory_space=pltpu.VMEM)
        results = pl.pallas_call(
            functools.partial(gather_kernel, ny, nz, nx, rows),
            out_shape=(
                pltpu.VMEM((n, total_rows, width), bf16),
                pltpu.VMEM((experts, rows), f32),
                pltpu.VMEM((ep * experts, n * width), bf16),
                pltpu.VMEM((total_rows, width), f32),
            ),
            in_specs=[pl.BlockSpec(memory_space=pltpu.HBM)] * 4,
            out_specs=(in_vmem,) * 4,
            scratch_shapes=[
                vmem((total_rows, width), f32),
                vmem((total_rows, width), f32),
                vmem((experts, width), f32),
                vmem((1, width), f32),
                vmem((n, total_rows * EARLY // CHUNKS, width), bf16),
                vmem((n, vregs + 1, 8, LANES), f32),
                vmem((2, vregs, 8, LANES), f32),
                vmem((n, -(-total_rows * EARLY // CHUNKS // (8 * LANES)), 8, LANES), f32),
                vmem((nz, nx, n, experts, width), f32),
                dma(2 * CHUNKS + 2),
                dma(2, half),
                dma(2, half),
                dma(2, half),
                dma(2, half, CHUNKS),
                dma(ny),
                dma(ny),
                dma(ny),
                dma(ny),
                dma(ny),
                dma(ny),
                dma(2, nz // 2 + 1),
                dma(2, nz // 2 + 1),
                dma(2, nx // 2 + 1),
                dma(2, nx // 2 + 1),
            ],
            compiler_params=pltpu.CompilerParams(
                collective_id=0, has_side_effects=True, vmem_limit_bytes=24 * 1024 * 1024
            ),
            name="gather",
        )(
            *(
                pltpu.with_memory_space_constraint(a, pltpu.HBM)
                for a in (
                    train_down.reshape(total_rows, width),
                    other_down.reshape(total_rows, width),
                    router_weight.T,
                    router_gain.reshape(1, width),
                )
            )
        )
        held = [pltpu.with_memory_space_constraint(r, pltpu.VMEM) for r in results]
        ready, scale, router, latest = pl.pallas_call(
            write_kernel,
            out_shape=(
                jax.ShapeDtypeStruct((total_rows, n * width), bf16),
                jax.ShapeDtypeStruct((experts, rows), f32),
                jax.ShapeDtypeStruct((ep * experts, n * width), bf16),
                jax.ShapeDtypeStruct((total_rows, width), f32),
            ),
            in_specs=[in_vmem] * 4,
            out_specs=(anywhere,) * 4,
            scratch_shapes=[dma(n + 3)],
            compiler_params=pltpu.CompilerParams(vmem_limit_bytes=1024 * 1024),
            name="write",
        )(*held)
        return (
            ready.reshape(experts, rows, n * width),
            scale,
            router.T,
            latest.reshape(experts, rows, width),
        )

    placed = (P("ep", None, "fsdp"), P("ep", None, "fsdp"), P("fsdp", "ep"), P("fsdp"))
    return jax.shard_map(
        on_device,
        mesh=mesh,
        in_specs=placed,
        out_specs=(P("ep", None, None), P("ep", None), P(), P("ep", None, "fsdp")),
        check_vma=False,
    )
```

```python
import functools

import jax
import jax.numpy as jnp
from jax import lax
from jax.experimental import pallas as pl
from jax.experimental.pallas import tpu as pltpu
from jax.sharding import PartitionSpec as P

MESH = pl.DeviceIdType.MESH
LANES = 128
CHUNKS = 16
EARLY = 6
RANGE = 240.0
TINY = 1e-36
TURNS = (6, 9, 12, 15, 16, 22, 28)
LN2 = 0.6931471805599453


def gather_kernel(
    ny, nz, nx, rows,
    train_ref, other_ref, weight_ref, gain_ref,
    land, scale_ref, router_ref, latest_ref,
    train_buf, other_buf, w_buf, g_buf, code, sums, inverse, factor, rland, load_sem, sum_send, sum_recv, ring_send, ring_recv,
    twin_send, twin_recv, tsum_send, tsum_recv, tcode_send, tcode_recv, z_send, z_recv, x_send, x_recv, here_sem,
):
    n = 2 * ny
    half = ny // 2
    total_rows = 2 * rows
    span = total_rows // CHUNKS
    early_rows = EARLY * span
    groups = total_rows // 8
    vregs = (groups + LANES - 1) // LANES
    f_me = lax.axis_index("fsdp")
    e_me = lax.axis_index("ep")
    y, core = f_me // 2, lax.rem(f_me, 2)
    z, x = e_me // nx, lax.rem(e_me, nx)

    def column(y_index, core_index):
        return {"fsdp": y_index * 2 + core_index}

    right = column(lax.rem(y + 1, ny), core)
    left = column(lax.rem(y + ny - 1, ny), core)
    twin = column(y, 1 - core)
    z_next = {"ep": lax.rem(z + 1, nz) * nx + x}
    z_last = {"ep": lax.rem(z + nz - 1, nz) * nx + x}
    x_next = {"ep": z * nx + lax.rem(x + 1, nx)}
    x_last = {"ep": z * nx + lax.rem(x + nx - 1, nx)}
    line = [right, left, twin]
    across = []
    if nz > 1:
        across += [(z_next, lax.rem(z + 1, nz), z, 0), (z_last, lax.rem(z + nz - 1, nz), z, 0)]
    if nx > 1:
        across += [(x_next, lax.rem(x + 1, nx), x, 1), (x_last, lax.rem(x + nx - 1, nx), x, 1)]

    small = (
        pltpu.make_async_copy(weight_ref, w_buf, load_sem.at[2 * CHUNKS]),
        pltpu.make_async_copy(gain_ref, g_buf, load_sem.at[2 * CHUNKS + 1]),
    )
    loads = []
    barrier = pltpu.get_barrier_semaphore()
    for k in range(CHUNKS):
        at = pl.ds(k * span, span)
        a = pltpu.make_async_copy(train_ref.at[at], train_buf.at[at], load_sem.at[2 * k])
        b = pltpu.make_async_copy(other_ref.at[at], other_buf.at[at], load_sem.at[2 * k + 1])
        a.start()
        b.start()
        loads.append((a, b))
        if k == 0:
            for p in line:
                pl.semaphore_signal(barrier, inc=1, device_id=p, device_id_type=MESH)
    for c in small:
        c.start()
    for p, there, here, _ in across:

        @pl.when(there > here)
        def _(p=p):
            pl.semaphore_signal(barrier, inc=1, device_id=p, device_id_type=MESH)


    def origin_of(way, hop):
        return lax.rem(y + (ny - hop if way == 0 else hop), ny)

    def apart(way, hop):
        return 0 if hop == 0 else (ny - hop if way == 0 else hop)

    def piece(k, origin, early):
        buf = code if early else land
        return buf.at[2 * origin + core, pl.ds(pl.multiple_of(k * span, 16), span)]

    def ring_copy(way, hop, k, early):
        block = piece(k, origin_of(way, hop - 1), early)
        return pltpu.make_async_remote_copy(
            block, block, ring_send.at[way, hop - 1], ring_recv.at[way, hop - 1, k],
            device_id=right if way == 0 else left, device_id_type=MESH,
        )

    def ring_wait(way, hop, k, early):
        block = piece(k, origin_of(way, hop), early)
        pltpu.make_async_remote_copy(
            block, block, ring_send.at[way, hop - 1], ring_recv.at[way, hop - 1, k],
            device_id=right if way == 0 else left, device_id_type=MESH,
        ).wait_recv()

    def twin_copy(way, hop, k, early):
        block = piece(k, origin_of(way, hop), early)
        d = apart(way, hop)
        return pltpu.make_async_remote_copy(
            block, block, (tcode_send if early else twin_send).at[d], (tcode_recv if early else twin_recv).at[d],
            device_id=twin, device_id_type=MESH,
        )

    def launch(k, early):
        ring_copy(0, 1, k, early).start()
        ring_copy(1, 1, k, early).start()
        twin_copy(0, 0, k, early).start()

    def arrival(way, hop, k, early, onward):
        ring_wait(way, hop, k, early)
        if onward:
            ring_copy(way, hop + 1, k, early).start()
        twin_copy(way, hop, k, early).start()

    def sum_copy(way, hop):
        block = sums.at[2 * origin_of(way, hop - 1) + core]
        return pltpu.make_async_remote_copy(
            block, block, sum_send.at[way, hop - 1], sum_recv.at[way, hop - 1],
            device_id=right if way == 0 else left, device_id_type=MESH,
        )

    def sum_wait(way, hop):
        block = sums.at[2 * origin_of(way, hop) + core]
        pltpu.make_async_remote_copy(
            block, block, sum_send.at[way, hop - 1], sum_recv.at[way, hop - 1],
            device_id=right if way == 0 else left, device_id_type=MESH,
        ).wait_recv()

    def sum_twin(d, whose):
        block = sums.at[2 * lax.rem(y + d, ny) + whose]
        return pltpu.make_async_remote_copy(
            block, block, tsum_send.at[d], tsum_recv.at[d], device_id=twin, device_id_type=MESH,
        )

    lane = lax.broadcasted_iota(jnp.int32, (8, LANES), 1)
    ones = jnp.ones((8, LANES), jnp.float32)
    words = [ones]

    def sweep(k):
        for c in loads[k]:
            c.wait()
        both = []
        for g in range(k * span // 8, (k + 1) * span // 8):
            at = pl.ds(g * 8, 8)
            value = 0.5 * other_buf[at, :] + 0.5 * train_buf[at, :]
            latest_ref[at, :] = value
            total = jnp.sum(value * value, axis=1, keepdims=True)
            words[0] = jnp.where(lane == g % LANES, total, words[0])
            if g % LANES == LANES - 1 or g == groups - 1:
                sums[f_me, g // LANES] = words[0]
                words[0] = ones
            if k < EARLY:
                reach = RANGE * lax.rsqrt(jnp.maximum(jnp.broadcast_to(total, (8, LANES)), TINY))
                size = jnp.exp(LN2 * (jnp.abs(value) * reach - RANGE / 2))
                both.append(jnp.where(value < 0, -size, size))
                if len(both) == 2:
                    code[f_me, pl.ds((g - 1) * 8, 16), :] = jnp.concatenate(both, axis=0).astype(jnp.bfloat16)
                    both = []

    sweep(0)
    lower = [jnp.where(there < here, 1, 0) for _, there, here, _ in across]
    pl.semaphore_wait(barrier, sum(lower, len(line)))
    launch(0, True)
    for p, there, here, axis in across:

        @pl.when(there < here)
        def _(p=p, axis=axis):
            pl.semaphore_signal(here_sem.at[axis], inc=1, device_id=p, device_id_type=MESH)

    sweep(1)
    launch(1, True)
    for k in range(2, CHUNKS):
        sweep(k)
        if k == 2:
            for c in small:
                c.wait()
            sums[f_me, vregs, pl.ds(0, 2), :] = w_buf[...] * g_buf[...]
    sum_copy(0, 1).start()
    sum_copy(1, 1).start()
    sum_twin(0, core).start()
    for k in range(2, min(4, EARLY)):
        launch(k, True)

    mid = EARLY // 2

    def early_step(hop, k):
        last = hop == half - 1
        arrival(0, hop, k, True, not last or k < mid)
        arrival(1, hop, k, True, not last or k >= mid)

    waiting = [(0, k) for k in range(4, EARLY)] + [(hop, k) for hop in range(1, half) for k in range(EARLY)]

    ahead = []

    def early_some(count):
        ahead.extend(waiting[:count])
        for hop, k in waiting[:count]:
            if hop == 0:
                launch(k, True)
            else:
                early_step(hop, k)
        del waiting[:count]

    for hop in range(1, half + 1):
        sum_wait(0, hop)
        if hop < half:
            sum_copy(0, hop + 1).start()
            sum_wait(1, hop)
            if hop < half - 1:
                sum_copy(1, hop + 1).start()
            sum_twin(apart(1, hop), core).start()
        sum_twin(apart(0, hop), core).start()
        early_some(3)
    for d in range(ny):
        sum_twin(d, 1 - core).wait_recv()

    for v in range(vregs):
        total = sums[0, v]
        for s in range(1, n):
            total = total + sums[s, v]
        scale = jnp.sqrt(total)
        inverse[0, v] = scale
        inverse[1, v] = 1.0 / scale

    def scaled(r):
        both = []
        for g in (2 * r, 2 * r + 1):
            inv = inverse[1, g // LANES][:, g % LANES : g % LANES + 1]
            both.append(latest_ref[pl.ds(8 * g, 8), :] * jnp.broadcast_to(inv, (8, LANES)))
        land[f_me, pl.ds(16 * r, 16), :] = jnp.concatenate(both, axis=0).astype(jnp.bfloat16)

    for k in range(EARLY, CHUNKS):
        for r in range(k * span // 16, (k + 1) * span // 16):
            scaled(r)
        launch(k, False)
    sent = {(hop + 1, k) for hop, k in ahead}
    first = [(hop, k) for hop, k in waiting if hop == 1 or (hop, k) in sent]
    second = [step for step in waiting if step not in first]
    for hop, k in first:
        early_step(hop, k)

    for f in range(n):
        rland[z, x, f] = sums[f, vregs, pl.ds(0, 2), :]

    def z_copy(way, step, where):
        block = rland.at[where, x]
        return pltpu.make_async_remote_copy(
            block, block, z_send.at[way, step], z_recv.at[way, step],
            device_id=z_last if way else z_next, device_id_type=MESH,
        )

    def x_copy(way, step, where):
        block = rland.at[:, where]
        return pltpu.make_async_remote_copy(
            block, block, x_send.at[way, step], x_recv.at[way, step],
            device_id=x_last if way else x_next, device_id_type=MESH,
        )

    def round_step(copy, size, me, step):
        for way, hops in enumerate((size // 2, size - 1 - size // 2)):
            where = lax.rem(me + size + (step if way else -step), size)
            if 1 <= step <= hops:
                copy(way, step - 1, where).wait_recv()
            if step < hops:
                copy(way, step, where).start()

    tasks = [functools.partial(round_step, z_copy, nz, z, step) for step in range(nz // 2 + 1)]
    tasks += [functools.partial(round_step, x_copy, nx, x, step) for step in range(nx // 2 + 1)]

    for s in range(n):
        for v in range(factor.shape[1]):
            factor[s, v] = jnp.sqrt(jnp.maximum(sums[s, v], TINY)) * inverse[1, v] * (1.0 / RANGE)
    for r in range(early_rows // 16):
        scaled(r)
    for axis in range(2):
        higher = [jnp.where(there > here, 1, 0) for _, there, here, a in across if a == axis]
        if higher:

            @pl.when(sum(higher) > 0)
            def _(axis=axis, count=sum(higher)):
                pl.semaphore_wait(here_sem.at[axis], count)

    tasks.pop(0)()

    def decode(i):
        far = ((i >= ny - 2) & (i < 2 * ny - 3)) | (i == 2 * ny - 2)
        near = jnp.where(far, i - (ny - 2), i + 1)
        offset = jnp.where(i >= 2 * ny - 3, half, near + jnp.where(near >= half, 1, 0))
        slot = 2 * lax.rem(y + offset, ny) + jnp.where(far, 1 - core, core)

        @pl.when(far)
        def _():
            block = code.at[slot]
            pltpu.make_async_remote_copy(
                block, block, tcode_send.at[offset], tcode_recv.at[offset], device_id=twin, device_id_type=MESH,
            ).wait_recv()

        by = [factor[slot, v] for v in range(factor.shape[1])]
        for r in range(early_rows // 16):
            held = code[slot, pl.ds(16 * r, 16), :].astype(jnp.float32)
            size = jnp.log(jnp.abs(held)) * (1.0 / LN2) + RANGE / 2
            signed = jnp.where(held < 0, -size, size)
            part = jnp.concatenate(
                [
                    jnp.broadcast_to(by[g // LANES][:, g % LANES : g % LANES + 1], (8, LANES))
                    for g in (2 * r, 2 * r + 1)
                ],
                axis=0,
            )
            land[slot, pl.ds(16 * r, 16), :] = (signed * part).astype(jnp.bfloat16)

    late = CHUNKS - EARLY
    turn = EARLY + late // 2
    codes = n - 1

    def pair(hop, k, extra):
        if hop < half - 1:
            arrival(0, hop, k, False, True)
            arrival(1, hop, k, False, True)
        else:
            for way in range(2):
                ring_wait(way, hop, k, False)
                twin_copy(way, hop, k, False).start()

            @pl.when(k < turn)
            def _():
                ring_copy(0, hop + 1, k, False).start()

            @pl.when(k >= turn)
            def _():
                ring_copy(1, hop + 1, k, False).start()
        extra(k)

    def decode_step(base):
        def run(k):
            i = base + k - EARLY

            @pl.when(i < codes)
            def _():
                decode(i)

        return run

    due = {}
    for i, task in enumerate(tasks):
        if half == 1 or i >= len(TURNS):
            due.setdefault((half - 1, CHUNKS - 1), []).append(task)
        else:
            hop, k = divmod(TURNS[i], late)
            due.setdefault((min(hop + 1, half - 1), k + EARLY), []).append(task)

    for hop in range(1, half):

        def extra(k, hop=hop):
            for (at_hop, at), todo in due.items():
                if at_hop == hop:

                    @pl.when(k == at)
                    def _(todo=todo):
                        for task in todo:
                            task()

            if hop > 1:
                decode_step(late * (hop - 2))(k)

        def body(k, c, hop=hop, extra=extra):
            pair(hop, k, extra)
            return c

        lax.fori_loop(EARLY, CHUNKS, body, 0)
        if hop == 1:
            for early_hop, k in second:
                early_step(early_hop, k)
        if hop == min(2, half - 1):
            for k in range(mid):
                arrival(0, half, k, True, False)
                arrival(1, half, k + mid, True, False)
        if hop == 1:
            rows_at = lax.broadcasted_iota(jnp.int32, (LANES, LANES), 0)
            lanes_at = lax.broadcasted_iota(jnp.int32, (LANES, LANES), 1)
            for t in range(total_rows // LANES):
                tile = jnp.concatenate(
                    [
                        jnp.broadcast_to(inverse[0, g // LANES][:, g % LANES : g % LANES + 1], (8, LANES))
                        for g in range(16 * t, 16 * t + 16)
                    ],
                    axis=0,
                )
                line = jnp.sum(jnp.where(rows_at == lanes_at, tile, 0.0), axis=0, keepdims=True)
                e, at = divmod(t * LANES, rows)
                scale_ref[pl.ds(e, 1), pl.ds(at, LANES)] = line
    for i in range(late * (half - 2), codes):
        decode(jnp.int32(i))

    def lines(f, c):
        for q in range(nz * nx // 8):
            block = jnp.concatenate([rland[(8 * q + i) // nx, (8 * q + i) % nx, f] for i in range(8)], axis=0)
            router_ref[pl.ds(16 * q, 16), pl.ds(pl.multiple_of(f * LANES, LANES), LANES)] = block.astype(jnp.bfloat16)
        return c

    lax.fori_loop(0, n, lines, 0)

    def final(k, c):
        arrival(0, half, k, False, False)
        arrival(1, half, k + late // 2, False, False)
        return c

    lax.fori_loop(EARLY, turn, final, 0)

    def whole(buf, send, recv, part_rows):
        block = buf.at[0, pl.ds(0, part_rows)]
        return pltpu.make_async_remote_copy(block, block, send, recv, device_id=twin, device_id_type=MESH)

    for way in range(2):
        for hop in range(1, half + 1):
            part_rows = total_rows if hop < half else total_rows // 2
            whole(land, ring_send.at[way, hop - 1], twin_recv.at[0], part_rows).wait_send()
    for way in range(2):
        for hop in range(1, half + 1 - way):
            sum_copy(way, hop).wait_send()
    for d in range(ny):
        sum_twin(d, core).wait_send()
        whole(code, tcode_send.at[d], tcode_recv.at[d], early_rows).wait_send()
    for copy, size, me in ((z_copy, nz, z), (x_copy, nx, x)):
        for way, hops in enumerate((size // 2, size - 1 - size // 2)):
            for step in range(hops):
                copy(way, step, me).wait_send()
    for d in range(ny):
        whole(land, twin_send.at[d], twin_recv.at[d], total_rows - early_rows).wait()


def write_kernel(land, scale_in, router_in, latest_in, ready, scale, router, latest, sem):
    n = land.shape[0]
    copies = [
        pltpu.make_async_copy(land.at[f], ready.at[:, pl.ds(f * LANES, LANES)], sem.at[f]) for f in range(n)
    ]
    copies.append(pltpu.make_async_copy(scale_in, scale, sem.at[n]))
    copies.append(pltpu.make_async_copy(router_in, router, sem.at[n + 1]))
    copies.append(pltpu.make_async_copy(latest_in, latest, sem.at[n + 2]))
    for c in copies:
        c.start()
    for c in copies:
        c.wait()


def solution(mesh, nx=4):
    ep, n = mesh.shape["ep"], mesh.shape["fsdp"]
    ny, nz = n // 2, ep // nx

    def on_device(train_down, other_down, router_weight, router_gain):
        experts, rows, width = train_down.shape
        total_rows = experts * rows
        vregs = (total_rows // 8 + LANES - 1) // LANES
        f32, bf16 = jnp.float32, jnp.bfloat16
        half = ny // 2
        vmem = lambda shape, dtype: pltpu.VMEM(shape, dtype)
        dma = lambda *shape: pltpu.SemaphoreType.DMA(shape)
        anywhere = pl.BlockSpec(memory_space=pl.ANY)
        in_vmem = pl.BlockSpec(memory_space=pltpu.VMEM)
        results = pl.pallas_call(
            functools.partial(gather_kernel, ny, nz, nx, rows),
            out_shape=(
                pltpu.VMEM((n, total_rows, width), bf16),
                pltpu.VMEM((experts, rows), f32),
                pltpu.VMEM((ep * experts, n * width), bf16),
                pltpu.VMEM((total_rows, width), f32),
            ),
            in_specs=[pl.BlockSpec(memory_space=pltpu.HBM)] * 4,
            out_specs=(in_vmem,) * 4,
            scratch_shapes=[
                vmem((total_rows, width), f32),
                vmem((total_rows, width), f32),
                vmem((experts, width), f32),
                vmem((1, width), f32),
                vmem((n, total_rows * EARLY // CHUNKS, width), bf16),
                vmem((n, vregs + 1, 8, LANES), f32),
                vmem((2, vregs, 8, LANES), f32),
                vmem((n, -(-total_rows * EARLY // CHUNKS // (8 * LANES)), 8, LANES), f32),
                vmem((nz, nx, n, experts, width), f32),
                dma(2 * CHUNKS + 2),
                dma(2, half),
                dma(2, half),
                dma(2, half),
                dma(2, half, CHUNKS),
                dma(ny),
                dma(ny),
                dma(ny),
                dma(ny),
                dma(ny),
                dma(ny),
                dma(2, nz // 2 + 1),
                dma(2, nz // 2 + 1),
                dma(2, nx // 2 + 1),
                dma(2, nx // 2 + 1),
                pltpu.SemaphoreType.REGULAR((2,)),
            ],
            compiler_params=pltpu.CompilerParams(
                collective_id=0, has_side_effects=True, vmem_limit_bytes=24 * 1024 * 1024
            ),
            name="gather",
        )(
            *(
                pltpu.with_memory_space_constraint(a, pltpu.HBM)
                for a in (
                    train_down.reshape(total_rows, width),
                    other_down.reshape(total_rows, width),
                    router_weight.T,
                    router_gain.reshape(1, width),
                )
            )
        )
        held = [pltpu.with_memory_space_constraint(r, pltpu.VMEM) for r in results]
        ready, scale, router, latest = pl.pallas_call(
            write_kernel,
            out_shape=(
                jax.ShapeDtypeStruct((total_rows, n * width), bf16),
                jax.ShapeDtypeStruct((experts, rows), f32),
                jax.ShapeDtypeStruct((ep * experts, n * width), bf16),
                jax.ShapeDtypeStruct((total_rows, width), f32),
            ),
            in_specs=[in_vmem] * 4,
            out_specs=(anywhere,) * 4,
            scratch_shapes=[dma(n + 3)],
            compiler_params=pltpu.CompilerParams(vmem_limit_bytes=1024 * 1024),
            name="write",
        )(*held)
        return (
            ready.reshape(experts, rows, n * width),
            scale,
            router.T,
            latest.reshape(experts, rows, width),
        )

    placed = (P("ep", None, "fsdp"), P("ep", None, "fsdp"), P("fsdp", "ep"), P("fsdp"))
    return jax.shard_map(
        on_device,
        mesh=mesh,
        in_specs=placed,
        out_specs=(P("ep", None, None), P("ep", None), P(), P("ep", None, "fsdp")),
        check_vma=False,
    )
```

```python
import functools

import jax
import jax.numpy as jnp
from jax import lax
from jax.experimental import pallas as pl
from jax.experimental.pallas import tpu as pltpu
from jax.sharding import PartitionSpec as P

MESH = pl.DeviceIdType.MESH
LANES = 128
CHUNKS = 16
EARLY = 6
RANGE = 240.0
TINY = 1e-36
TURNS = (6, 9, 12, 15, 16, 22, 28)
LN2 = 0.6931471805599453


def gather_kernel(
    ny, nz, nx, rows,
    train_ref, other_ref, weight_ref, gain_ref,
    land, scale_ref, router_ref, latest_ref,
    train_buf, other_buf, w_buf, g_buf, code, sums, inverse, factor, rland, load_sem, sum_send, sum_recv, ring_send, ring_recv,
    twin_send, twin_recv, tsum_send, tsum_recv, tcode_send, tcode_recv, z_send, z_recv, x_send, x_recv, here_sem,
):
    n = 2 * ny
    half = ny // 2
    total_rows = 2 * rows
    span = total_rows // CHUNKS
    early_rows = EARLY * span
    groups = total_rows // 8
    vregs = (groups + LANES - 1) // LANES
    f_me = lax.axis_index("fsdp")
    e_me = lax.axis_index("ep")
    y, core = f_me // 2, lax.rem(f_me, 2)
    z, x = e_me // nx, lax.rem(e_me, nx)

    def column(y_index, core_index):
        return {"fsdp": y_index * 2 + core_index}

    right = column(lax.rem(y + 1, ny), core)
    left = column(lax.rem(y + ny - 1, ny), core)
    twin = column(y, 1 - core)
    z_next = {"ep": lax.rem(z + 1, nz) * nx + x}
    z_last = {"ep": lax.rem(z + nz - 1, nz) * nx + x}
    x_next = {"ep": z * nx + lax.rem(x + 1, nx)}
    x_last = {"ep": z * nx + lax.rem(x + nx - 1, nx)}
    line = [right, left, twin]
    across = []
    if nz > 1:
        across += [(z_next, lax.rem(z + 1, nz), z, 0), (z_last, lax.rem(z + nz - 1, nz), z, 0)]
    if nx > 1:
        across += [(x_next, lax.rem(x + 1, nx), x, 1), (x_last, lax.rem(x + nx - 1, nx), x, 1)]

    small = (
        pltpu.make_async_copy(weight_ref, w_buf, load_sem.at[2 * CHUNKS]),
        pltpu.make_async_copy(gain_ref, g_buf, load_sem.at[2 * CHUNKS + 1]),
    )
    loads = []
    barrier = pltpu.get_barrier_semaphore()
    for k in range(CHUNKS):
        at = pl.ds(k * span, span)
        a = pltpu.make_async_copy(train_ref.at[at], train_buf.at[at], load_sem.at[2 * k])
        b = pltpu.make_async_copy(other_ref.at[at], other_buf.at[at], load_sem.at[2 * k + 1])
        a.start()
        b.start()
        loads.append((a, b))
        if k == 0:
            for p in line:
                pl.semaphore_signal(barrier, inc=1, device_id=p, device_id_type=MESH)
    for c in small:
        c.start()
    for p, there, here, _ in across:

        @pl.when(there > here)
        def _(p=p):
            pl.semaphore_signal(barrier, inc=1, device_id=p, device_id_type=MESH)


    def origin_of(way, hop):
        return lax.rem(y + (ny - hop if way == 0 else hop), ny)

    def apart(way, hop):
        return 0 if hop == 0 else (ny - hop if way == 0 else hop)

    def piece(k, origin, early):
        buf = code if early else land
        return buf.at[2 * origin + core, pl.ds(pl.multiple_of(k * span, 16), span)]

    def ring_copy(way, hop, k, early):
        block = piece(k, origin_of(way, hop - 1), early)
        return pltpu.make_async_remote_copy(
            block, block, ring_send.at[way, hop - 1], ring_recv.at[way, hop - 1, k],
            device_id=right if way == 0 else left, device_id_type=MESH,
        )

    def ring_wait(way, hop, k, early):
        block = piece(k, origin_of(way, hop), early)
        pltpu.make_async_remote_copy(
            block, block, ring_send.at[way, hop - 1], ring_recv.at[way, hop - 1, k],
            device_id=right if way == 0 else left, device_id_type=MESH,
        ).wait_recv()

    def twin_copy(way, hop, k, early):
        block = piece(k, origin_of(way, hop), early)
        d = apart(way, hop)
        return pltpu.make_async_remote_copy(
            block, block, (tcode_send if early else twin_send).at[d], (tcode_recv if early else twin_recv).at[d],
            device_id=twin, device_id_type=MESH,
        )

    def launch(k, early):
        ring_copy(0, 1, k, early).start()
        ring_copy(1, 1, k, early).start()
        twin_copy(0, 0, k, early).start()

    def arrival(way, hop, k, early, onward):
        ring_wait(way, hop, k, early)
        if onward:
            ring_copy(way, hop + 1, k, early).start()
        twin_copy(way, hop, k, early).start()

    def sum_copy(way, hop):
        block = sums.at[2 * origin_of(way, hop - 1) + core]
        return pltpu.make_async_remote_copy(
            block, block, sum_send.at[way, hop - 1], sum_recv.at[way, hop - 1],
            device_id=right if way == 0 else left, device_id_type=MESH,
        )

    def sum_wait(way, hop):
        block = sums.at[2 * origin_of(way, hop) + core]
        pltpu.make_async_remote_copy(
            block, block, sum_send.at[way, hop - 1], sum_recv.at[way, hop - 1],
            device_id=right if way == 0 else left, device_id_type=MESH,
        ).wait_recv()

    def sum_twin(d, whose):
        block = sums.at[2 * lax.rem(y + d, ny) + whose]
        return pltpu.make_async_remote_copy(
            block, block, tsum_send.at[d], tsum_recv.at[d], device_id=twin, device_id_type=MESH,
        )

    lane = lax.broadcasted_iota(jnp.int32, (8, LANES), 1)
    ones = jnp.ones((8, LANES), jnp.float32)
    words = [ones]

    def sweep(k):
        for c in loads[k]:
            c.wait()
        both = []
        for g in range(k * span // 8, (k + 1) * span // 8):
            at = pl.ds(g * 8, 8)
            value = 0.5 * other_buf[at, :] + 0.5 * train_buf[at, :]
            latest_ref[at, :] = value
            total = jnp.sum(value * value, axis=1, keepdims=True)
            words[0] = jnp.where(lane == g % LANES, total, words[0])
            if g % LANES == LANES - 1 or g == groups - 1:
                sums[f_me, g // LANES] = words[0]
                words[0] = ones
            if k < EARLY:
                reach = RANGE * lax.rsqrt(jnp.maximum(jnp.broadcast_to(total, (8, LANES)), TINY))
                size = jnp.exp(LN2 * (jnp.abs(value) * reach - RANGE / 2))
                both.append(jnp.where(value < 0, -size, size))
                if len(both) == 2:
                    code[f_me, pl.ds((g - 1) * 8, 16), :] = jnp.concatenate(both, axis=0).astype(jnp.bfloat16)
                    both = []

    sweep(0)
    lower = [jnp.where(there < here, 1, 0) for _, there, here, _ in across]
    pl.semaphore_wait(barrier, sum(lower, len(line)))
    launch(0, True)
    for p, there, here, axis in across:

        @pl.when(there < here)
        def _(p=p, axis=axis):
            pl.semaphore_signal(here_sem.at[axis], inc=1, device_id=p, device_id_type=MESH)

    sweep(1)
    launch(1, True)
    for k in range(2, CHUNKS):
        sweep(k)
        if k == 2:
            for c in small:
                c.wait()
            sums[f_me, vregs, pl.ds(0, 2), :] = w_buf[...] * g_buf[...]
    sum_copy(0, 1).start()
    sum_copy(1, 1).start()
    sum_twin(0, core).start()
    for k in range(2, min(4, EARLY)):
        launch(k, True)

    mid = EARLY // 2

    def early_step(hop, k):
        last = hop == half - 1
        arrival(0, hop, k, True, not last or k < mid)
        arrival(1, hop, k, True, not last or k >= mid)

    waiting = [(0, k) for k in range(4, EARLY)] + [(hop, k) for hop in range(1, half) for k in range(EARLY)]

    ahead = []

    def early_some(count):
        ahead.extend(waiting[:count])
        for hop, k in waiting[:count]:
            if hop == 0:
                launch(k, True)
            else:
                early_step(hop, k)
        del waiting[:count]

    for hop in range(1, half + 1):
        sum_wait(0, hop)
        if hop < half:
            sum_copy(0, hop + 1).start()
            sum_wait(1, hop)
            if hop < half - 1:
                sum_copy(1, hop + 1).start()
            sum_twin(apart(1, hop), core).start()
        sum_twin(apart(0, hop), core).start()
        early_some(3)
    for d in range(ny):
        sum_twin(d, 1 - core).wait_recv()

    for v in range(vregs):
        total = sums[0, v]
        for s in range(1, n):
            total = total + sums[s, v]
        scale = jnp.sqrt(total)
        inverse[0, v] = scale
        inverse[1, v] = 1.0 / scale

    def scaled(r):
        both = []
        for g in (2 * r, 2 * r + 1):
            inv = inverse[1, g // LANES][:, g % LANES : g % LANES + 1]
            both.append(latest_ref[pl.ds(8 * g, 8), :] * jnp.broadcast_to(inv, (8, LANES)))
        land[f_me, pl.ds(16 * r, 16), :] = jnp.concatenate(both, axis=0).astype(jnp.bfloat16)

    for k in range(EARLY, CHUNKS):
        for r in range(k * span // 16, (k + 1) * span // 16):
            scaled(r)
        launch(k, False)
    sent = {(hop + 1, k) for hop, k in ahead}
    first = [(hop, k) for hop, k in waiting if hop == 1 or (hop, k) in sent]
    second = [step for step in waiting if step not in first]
    for hop, k in first:
        early_step(hop, k)

    for f in range(n):
        rland[z, x, f] = sums[f, vregs, pl.ds(0, 2), :]

    def z_copy(way, step, where):
        block = rland.at[where, x]
        return pltpu.make_async_remote_copy(
            block, block, z_send.at[way, step], z_recv.at[way, step],
            device_id=z_last if way else z_next, device_id_type=MESH,
        )

    def x_copy(way, step, where):
        block = rland.at[:, where]
        return pltpu.make_async_remote_copy(
            block, block, x_send.at[way, step], x_recv.at[way, step],
            device_id=x_last if way else x_next, device_id_type=MESH,
        )

    def round_step(copy, size, me, step):
        for way, hops in enumerate((size // 2, size - 1 - size // 2)):
            where = lax.rem(me + size + (step if way else -step), size)
            if 1 <= step <= hops:
                copy(way, step - 1, where).wait_recv()
            if step < hops:
                copy(way, step, where).start()

    tasks = [functools.partial(round_step, z_copy, nz, z, step) for step in range(nz // 2 + 1)]
    tasks += [functools.partial(round_step, x_copy, nx, x, step) for step in range(nx // 2 + 1)]

    for s in range(n):
        for v in range(factor.shape[1]):
            factor[s, v] = jnp.sqrt(jnp.maximum(sums[s, v], TINY)) * inverse[1, v] * (1.0 / RANGE)
    for r in range(early_rows // 16):
        scaled(r)
    for axis in range(2):
        higher = [jnp.where(there > here, 1, 0) for _, there, here, a in across if a == axis]
        if higher:

            @pl.when(sum(higher) > 0)
            def _(axis=axis, count=sum(higher)):
                pl.semaphore_wait(here_sem.at[axis], count)

    tasks.pop(0)()

    def decode(i):
        far = ((i >= ny - 2) & (i < 2 * ny - 3)) | (i == 2 * ny - 2)
        near = jnp.where(far, i - (ny - 2), i + 1)
        offset = jnp.where(i >= 2 * ny - 3, half, near + jnp.where(near >= half, 1, 0))
        slot = 2 * lax.rem(y + offset, ny) + jnp.where(far, 1 - core, core)

        @pl.when(far)
        def _():
            block = code.at[slot]
            pltpu.make_async_remote_copy(
                block, block, tcode_send.at[offset], tcode_recv.at[offset], device_id=twin, device_id_type=MESH,
            ).wait_recv()

        by = [factor[slot, v] for v in range(factor.shape[1])]
        for r in range(early_rows // 16):
            held = code[slot, pl.ds(16 * r, 16), :].astype(jnp.float32)
            size = jnp.log(jnp.abs(held)) * (1.0 / LN2) + RANGE / 2
            signed = jnp.where(held < 0, -size, size)
            part = jnp.concatenate(
                [
                    jnp.broadcast_to(by[g // LANES][:, g % LANES : g % LANES + 1], (8, LANES))
                    for g in (2 * r, 2 * r + 1)
                ],
                axis=0,
            )
            land[slot, pl.ds(16 * r, 16), :] = (signed * part).astype(jnp.bfloat16)

    late = CHUNKS - EARLY
    turn = EARLY + late // 2
    codes = n - 1

    def pair(hop, k, extra):
        if hop < half - 1:
            arrival(0, hop, k, False, True)
            arrival(1, hop, k, False, True)
        else:
            for way in range(2):
                ring_wait(way, hop, k, False)
                twin_copy(way, hop, k, False).start()

            @pl.when(k < turn)
            def _():
                ring_copy(0, hop + 1, k, False).start()

            @pl.when(k >= turn)
            def _():
                ring_copy(1, hop + 1, k, False).start()
        extra(k)

    def decode_step(base):
        def run(k):
            i = base + k - EARLY

            @pl.when(i < codes)
            def _():
                decode(i)

        return run

    due = {}
    for i, task in enumerate(tasks):
        if half == 1 or i >= len(TURNS):
            due.setdefault((half - 1, CHUNKS - 1), []).append(task)
        else:
            hop, k = divmod(TURNS[i], late)
            due.setdefault((min(hop + 1, half - 1), k + EARLY), []).append(task)

    for hop in range(1, half):

        def extra(k, hop=hop):
            for (at_hop, at), todo in due.items():
                if at_hop == hop:

                    @pl.when(k == at)
                    def _(todo=todo):
                        for task in todo:
                            task()

            if hop > 1:
                decode_step(late * (hop - 2))(k)

        def body(k, c, hop=hop, extra=extra):
            pair(hop, k, extra)
            return c

        lax.fori_loop(EARLY, CHUNKS, body, 0)
        if hop == 1:
            for early_hop, k in second:
                early_step(early_hop, k)
        if hop == min(2, half - 1):
            for k in range(mid):
                arrival(0, half, k, True, False)
                arrival(1, half, k + mid, True, False)
        if hop == 1:
            rows_at = lax.broadcasted_iota(jnp.int32, (LANES, LANES), 0)
            lanes_at = lax.broadcasted_iota(jnp.int32, (LANES, LANES), 1)
            for t in range(total_rows // LANES):
                tile = jnp.concatenate(
                    [
                        jnp.broadcast_to(inverse[0, g // LANES][:, g % LANES : g % LANES + 1], (8, LANES))
                        for g in range(16 * t, 16 * t + 16)
                    ],
                    axis=0,
                )
                line = jnp.sum(jnp.where(rows_at == lanes_at, tile, 0.0), axis=0, keepdims=True)
                e, at = divmod(t * LANES, rows)
                scale_ref[pl.ds(e, 1), pl.ds(at, LANES)] = line
    for i in range(late * (half - 2), codes):
        decode(jnp.int32(i))

    def lines(f, c):
        for q in range(nz * nx // 8):
            block = jnp.concatenate([rland[(8 * q + i) // nx, (8 * q + i) % nx, f] for i in range(8)], axis=0)
            router_ref[pl.ds(16 * q, 16), pl.ds(pl.multiple_of(f * LANES, LANES), LANES)] = block.astype(jnp.bfloat16)
        return c

    lax.fori_loop(0, n, lines, 0)

    def final(k, c):
        arrival(0, half, k, False, False)
        arrival(1, half, k + late // 2, False, False)
        return c

    lax.fori_loop(EARLY, turn, final, 0)

    def whole(buf, send, recv, part_rows):
        block = buf.at[0, pl.ds(0, part_rows)]
        return pltpu.make_async_remote_copy(block, block, send, recv, device_id=twin, device_id_type=MESH)

    for way in range(2):
        for hop in range(1, half + 1):
            part_rows = total_rows if hop < half else total_rows // 2
            whole(land, ring_send.at[way, hop - 1], twin_recv.at[0], part_rows).wait_send()
    for way in range(2):
        for hop in range(1, half + 1 - way):
            sum_copy(way, hop).wait_send()
    for d in range(ny):
        sum_twin(d, core).wait_send()
        whole(code, tcode_send.at[d], tcode_recv.at[d], early_rows).wait_send()
    for copy, size, me in ((z_copy, nz, z), (x_copy, nx, x)):
        for way, hops in enumerate((size // 2, size - 1 - size // 2)):
            for step in range(hops):
                copy(way, step, me).wait_send()
    for d in range(ny):
        whole(land, twin_send.at[d], twin_recv.at[d], total_rows - early_rows).wait()


def write_kernel(land, scale_in, router_in, latest_in, ready, scale, router, latest, sem):
    n = land.shape[0]
    copies = [
        pltpu.make_async_copy(land.at[f], ready.at[:, pl.ds(f * LANES, LANES)], sem.at[f]) for f in range(n)
    ]
    copies.append(pltpu.make_async_copy(scale_in, scale, sem.at[n]))
    copies.append(pltpu.make_async_copy(router_in, router, sem.at[n + 1]))
    copies.append(pltpu.make_async_copy(latest_in, latest, sem.at[n + 2]))
    for i, c in enumerate(copies):
        c.start(priority=i % 2)
    for c in copies:
        c.wait()


def solution(mesh, nx=4):
    ep, n = mesh.shape["ep"], mesh.shape["fsdp"]
    ny, nz = n // 2, ep // nx

    def on_device(train_down, other_down, router_weight, router_gain):
        experts, rows, width = train_down.shape
        total_rows = experts * rows
        vregs = (total_rows // 8 + LANES - 1) // LANES
        f32, bf16 = jnp.float32, jnp.bfloat16
        half = ny // 2
        vmem = lambda shape, dtype: pltpu.VMEM(shape, dtype)
        dma = lambda *shape: pltpu.SemaphoreType.DMA(shape)
        anywhere = pl.BlockSpec(memory_space=pl.ANY)
        in_vmem = pl.BlockSpec(memory_space=pltpu.VMEM)
        results = pl.pallas_call(
            functools.partial(gather_kernel, ny, nz, nx, rows),
            out_shape=(
                pltpu.VMEM((n, total_rows, width), bf16),
                pltpu.VMEM((experts, rows), f32),
                pltpu.VMEM((ep * experts, n * width), bf16),
                pltpu.VMEM((total_rows, width), f32),
            ),
            in_specs=[pl.BlockSpec(memory_space=pltpu.HBM)] * 4,
            out_specs=(in_vmem,) * 4,
            scratch_shapes=[
                vmem((total_rows, width), f32),
                vmem((total_rows, width), f32),
                vmem((experts, width), f32),
                vmem((1, width), f32),
                vmem((n, total_rows * EARLY // CHUNKS, width), bf16),
                vmem((n, vregs + 1, 8, LANES), f32),
                vmem((2, vregs, 8, LANES), f32),
                vmem((n, -(-total_rows * EARLY // CHUNKS // (8 * LANES)), 8, LANES), f32),
                vmem((nz, nx, n, experts, width), f32),
                dma(2 * CHUNKS + 2),
                dma(2, half),
                dma(2, half),
                dma(2, half),
                dma(2, half, CHUNKS),
                dma(ny),
                dma(ny),
                dma(ny),
                dma(ny),
                dma(ny),
                dma(ny),
                dma(2, nz // 2 + 1),
                dma(2, nz // 2 + 1),
                dma(2, nx // 2 + 1),
                dma(2, nx // 2 + 1),
                pltpu.SemaphoreType.REGULAR((2,)),
            ],
            compiler_params=pltpu.CompilerParams(
                collective_id=0, has_side_effects=True, vmem_limit_bytes=24 * 1024 * 1024
            ),
            name="gather",
        )(
            *(
                pltpu.with_memory_space_constraint(a, pltpu.HBM)
                for a in (
                    train_down.reshape(total_rows, width),
                    other_down.reshape(total_rows, width),
                    router_weight.T,
                    router_gain.reshape(1, width),
                )
            )
        )
        held = [pltpu.with_memory_space_constraint(r, pltpu.VMEM) for r in results]
        ready, scale, router, latest = pl.pallas_call(
            write_kernel,
            out_shape=(
                jax.ShapeDtypeStruct((total_rows, n * width), bf16),
                jax.ShapeDtypeStruct((experts, rows), f32),
                jax.ShapeDtypeStruct((ep * experts, n * width), bf16),
                jax.ShapeDtypeStruct((total_rows, width), f32),
            ),
            in_specs=[in_vmem] * 4,
            out_specs=(anywhere,) * 4,
            scratch_shapes=[dma(n + 3)],
            compiler_params=pltpu.CompilerParams(vmem_limit_bytes=1024 * 1024),
            name="write",
        )(*held)
        return (
            ready.reshape(experts, rows, n * width),
            scale,
            router.T,
            latest.reshape(experts, rows, width),
        )

    placed = (P("ep", None, "fsdp"), P("ep", None, "fsdp"), P("fsdp", "ep"), P("fsdp"))
    return jax.shard_map(
        on_device,
        mesh=mesh,
        in_specs=placed,
        out_specs=(P("ep", None, None), P("ep", None), P(), P("ep", None, "fsdp")),
        check_vma=False,
    )
```
